32 devices in a mesh: row: 4 (over y, x), col: 8 (over z, core).
Axes of the slice: x: 2, y: 2, z: 4, core: 2. Of those that a mesh axis runs over, the one named last changes fastest.
Arguments:
- operator: float32 [4096, 4096], P('row', 'col'), may hold values from -0.09375 to 0.09375
- state: float32 [4096, 4096], P('row', 'col'), may hold values from -60 to 60, as said below
- source: float32 [4096, 4096], P('row', 'col'), may hold values from -60 to 60, as said below
Outputs:
- state_next: float32 [4096, 4096], P('row', 'col')
- operator_fourth: float32 [4096, 4096], P('row', 'col')
The draws below stay inside these ranges and needn't reach their ends.
Inputs may be any that keep to these rules, and one draw needn't show every extreme that they name: symmetric: state equals its transpose. symmetric: source equals its transpose.
All inputs are finite; a program needn't handle non-finite values.
Results may differ from the reference program's by a relative error of at most 0.000098.
Values sent between devices are 32-bit elements; how exact they have to be, the bound alone decides.
No kernel may reach another device: no remote copies, remote signals or barrier semaphores. Data moves between devices by JAX's collectives and lax.ppermute only.
A program may use at most 128 MiB of HBM per device.

```python
import jax
import jax.numpy as jnp
from jax import lax

N = 4096


def symmetric_draw(key):
    base = jax.random.truncated_normal(key, -6.0, 6.0, (N, N), jnp.float32)
    return ((base + base.T) * 0.5).astype(jnp.float32)


def draw_state(key, part):
    return symmetric_draw(jax.random.fold_in(key, 11))


def draw_source(key, part):
    return symmetric_draw(jax.random.fold_in(key, 23))


def levels(key, shape, shards, low, top_value):
    factor_of, own = 1.0, jax.random.fold_in(key, 6)
    for axis_at, blocks in shards:
        steps = jnp.exp(jax.random.uniform(jax.random.fold_in(own, axis_at), (blocks,), jnp.float32, low / len(shards), top_value / len(shards)))
        factor_of = factor_of * jnp.repeat(steps, shape[axis_at] // blocks).reshape([-1 if axis == axis_at else 1 for axis in range(len(shape))])
    return factor_of


def gaussian(key, shape, deviation, bound, pieces=(), held_as=jnp.bfloat16):
    entries = jax.random.normal(key, shape, jnp.float32) * deviation
    if len(pieces) > 0:
        entries = levels(key, shape, pieces, -0.22, 0.18) * entries
    return jnp.clip(entries, min=-bound, max=bound).astype(held_as)


def setup_inputs(seed: int = 0) -> dict:
    streams_of = jax.random.split(jax.random.key(seed), 4)
    return {
        "operator": gaussian(streams_of[0], (N, N), N ** -0.5, 0.09375, ((0, 4), (1, 8)), jnp.float32),
        "state": draw_state(jax.random.fold_in(streams_of[3], 71), 0),
        "source": draw_source(jax.random.fold_in(streams_of[3], 71), 0),
    }


def matmul(left, right):
    return jnp.dot(left, right, preferred_element_type=jnp.float32, precision=lax.Precision.HIGHEST)


def reference(operator, state, source):
    product = matmul(operator, state)
    square = matmul(operator, operator)
    state_next = matmul(operator, product.T) + source
    operator_fourth = matmul(square, square)
    return state_next, operator_fourth
```

```python
import functools

import jax
import jax.numpy as jnp
from jax import lax
from jax.experimental import pallas as pl
from jax.experimental.pallas import tpu as pltpu
from jax.sharding import PartitionSpec as P


PIECES = 2
SENT = (1, 1)
TILE = 512


def halves(value):
    high = value.astype(jnp.bfloat16)
    return high, (value - high.astype(jnp.float32)).astype(jnp.bfloat16)


def wide(value):
    high, low = halves(value)
    return jnp.concatenate([high, high, low], axis=1)


def row_kernel(steps, pieces, joined, tile, at_ref, *rest):
    panels, rest = rest[: 2 * pieces], rest[2 * pieces :]
    blocks, rest = rest[: 2 * steps], rest[2 * steps :]
    rest, (left_ref, right_ref, tall_ref, sems) = rest[:-4], rest[-4:]
    count = 1 if joined else pieces
    starts, outs = rest[:-count], rest[-count:] * (pieces // count)
    core = at_ref[steps]
    depth = panels[0].shape[2]
    rows = panels[0].shape[1]
    tile = min(tile, rows)

    def place(half):
        return pl.ds(pl.multiple_of((core ^ half) * depth, depth), depth)

    def copies(step, slot, first, second):
        found = [
            pltpu.make_async_copy(first, right_ref.at[slot, place(0), :], sems.at[slot, 0]),
            pltpu.make_async_copy(second, right_ref.at[slot, place(1), :], sems.at[slot, 1]),
        ]
        for index, panel in enumerate(panels):
            begin, side = index // 2 * rows, index % 2 * depth
            found.append(
                pltpu.make_async_copy(
                    panel.at[at_ref[step]],
                    left_ref.at[slot, begin : begin + rows, side : side + depth],
                    sems.at[slot, 2 + index],
                )
            )
        return found

    def begin(step):
        for copy in copies(step, step % 2, blocks[2 * step], blocks[2 * step + 1]):
            copy.start()

    begin(0)

    @pl.loop(0, steps)
    def _(step):
        slot = step % 2
        waits = copies(step, slot, blocks[0], blocks[1])
        for copy in waits[:4]:
            copy.wait()
        for after in range(1, steps):
            pl.when(step == after - 1)(functools.partial(begin, after))
        chunk = min(128, 2 * depth)

        @pl.loop(0, 2 * depth // chunk)
        def _(index):
            begin = pl.multiple_of(index * chunk, chunk)
            high, low = halves(right_ref[slot, pl.ds(begin, chunk), :])
            tall_ref[pl.ds(begin, chunk), :] = high
            tall_ref[pl.ds(2 * depth + begin, chunk), :] = low
            tall_ref[pl.ds(4 * depth + begin, chunk), :] = high

        for piece in range(pieces):
            out_ref = outs[piece]
            for copy in waits[2 + 2 * piece : 4 + 2 * piece] if piece else ():
                copy.wait()

            @pl.loop(0, rows // tile)
            def _(index):
                at = pl.ds(pl.multiple_of(index * tile, tile), tile)
                here = pl.ds(pl.multiple_of(piece * rows + index * tile, tile), tile)
                to = here if joined else at
                part = jnp.dot(
                    wide(left_ref[slot, here, :]),
                    tall_ref[...],
                    preferred_element_type=jnp.float32,
                )

                @pl.when(step == 0)
                def _():
                    out_ref[to, :] = part + starts[piece][at, :] if starts else part

                @pl.when(step > 0)
                def _():
                    out_ref[to, :] += part


def row_product(panels, blocks, steps, starts=(), joined=False, tile=TILE):
    place, row = lax.axis_index("col"), lax.axis_index("row")
    chips, rows, depth = panels[0][0].shape
    rights = [half for step in steps for half in blocks[step]]
    count, pieces, width = len(steps), len(panels), rights[0].shape[1]
    order = jnp.arange(count + 1, dtype=jnp.int32) + steps[0]
    at = jnp.where(
        order == steps[0] + count, place % 2, ((order ^ row) - place // 2 + chips) % chips
    ).astype(jnp.int32)
    whole = pl.BlockSpec((rows, width), lambda step, at: (0, 0))
    shape = (pieces * rows if joined else rows, width)
    results = 1 if joined else pieces
    there = pl.BlockSpec(memory_space=pl.ANY)
    return pl.pallas_call(
        functools.partial(row_kernel, count, pieces, joined, tile),
        out_shape=[jax.ShapeDtypeStruct(shape, jnp.float32)] * results,
        grid_spec=pltpu.PrefetchScalarGridSpec(
            num_scalar_prefetch=1,
            grid=(1,),
            in_specs=[there] * (2 * pieces + 2 * count) + [whole] * len(starts),
            out_specs=[pl.BlockSpec(shape, lambda step, at: (0, 0))] * results,
            scratch_shapes=[
                pltpu.VMEM((2, pieces * rows, 2 * depth), jnp.float32),
                pltpu.VMEM((2, 2 * depth, width), jnp.float32),
                pltpu.VMEM((6 * depth, width), jnp.bfloat16),
                pltpu.SemaphoreType.DMA((2, 2 + 2 * pieces)),
            ],
        ),
        compiler_params=pltpu.CompilerParams(dimension_semantics=("arbitrary",)),
        cost_estimate=pl.CostEstimate(
            flops=12 * pieces * rows * width * depth * count,
            bytes_accessed=16 * count * depth * (pieces * rows + width),
            transcendentals=0,
        ),
    )(at, *(side for panel in panels for side in panel), *rights, *starts)


def term_kernel(steps, pieces, at_ref, own_ref, other_ref, kept_ref, came_ref, *rest):
    outs, left_ref = rest[:-1], rest[-1]
    turn = pl.program_id(0)

    @pl.when(turn == 0)
    def _():
        left_ref[...] = wide(jnp.concatenate([own_ref[...], other_ref[...]], axis=1))

    high, low = halves(jnp.concatenate([kept_ref[0], came_ref[0]], axis=1))
    part = lax.dot_general(
        left_ref[...],
        jnp.concatenate([high, low, high], axis=1),
        (((1,), (1,)), ((), ())),
        preferred_element_type=jnp.float32,
    )
    rows = outs[0].shape[0]
    for step in range(steps):

        @pl.when(turn == step)
        def _():
            for piece in range(pieces):
                outs[step * pieces + piece][...] = part[piece * rows : (piece + 1) * rows]


def term_products(product, turned, steps, pieces):
    own, other = product
    kept, came = turned
    place, row = lax.axis_index("col"), lax.axis_index("row")
    chips, width, depth = kept.shape
    rows = own.shape[0]
    at = (((place // 2 + jnp.array(steps, jnp.int32)) % chips) ^ row).astype(jnp.int32)
    whole = pl.BlockSpec((rows, depth), lambda step, at: (0, 0))
    shape = (rows // pieces, width)
    result = pl.BlockSpec(shape, lambda step, at: (0, 0))
    right = pl.BlockSpec((1, width, depth), lambda step, at: (at[step], 0, 0))
    return pl.pallas_call(
        functools.partial(term_kernel, len(steps), pieces),
        out_shape=[jax.ShapeDtypeStruct(shape, jnp.float32)] * (len(steps) * pieces),
        grid_spec=pltpu.PrefetchScalarGridSpec(
            num_scalar_prefetch=1,
            grid=(len(steps),),
            in_specs=[whole, whole, right, right],
            out_specs=[result] * (len(steps) * pieces),
            scratch_shapes=[pltpu.VMEM((rows, 6 * depth), jnp.bfloat16)],
        ),
        compiler_params=pltpu.CompilerParams(dimension_semantics=("arbitrary",)),
        cost_estimate=pl.CostEstimate(
            flops=12 * rows * width * depth * len(steps),
            bytes_accessed=12 * len(steps) * depth * (rows + width),
            transcendentals=0,
        ),
    )(at, own, other, kept, came)


def swap(value, bit):
    size = lax.axis_size("row")
    return lax.ppermute(value, "row", [(at, at ^ bit) for at in range(size)])


def partner(value):
    size = lax.axis_size("col")
    return lax.ppermute(value, "col", [(at, at ^ 1) for at in range(size)])


def spread(own):
    blocks = [own]
    for step in range(1, lax.axis_size("row")):
        low, high = step & -step, 1 << (step.bit_length() - 1)
        top = swap(blocks[step ^ low][0], low)
        bottom = swap(blocks[step ^ high][1], high)
        blocks.append((top, bottom))
    return blocks


def row_panels(parts):
    chips = lax.axis_size("col") // 2
    pieces = len(parts)
    ups = [[part] for part in parts]
    downs = [[part] for part in parts]
    for turn in range(1, chips):
        rise = [(at, at + 2) for at in range(2 * chips - 2) if at // 2 >= turn - 1]
        fall = [(at, at - 2) for at in range(2, 2 * chips) if at // 2 <= chips - turn]
        for piece in range(pieces):
            ups[piece].append(lax.ppermute(ups[piece][-1], "col", rise))
            downs[piece].append(lax.ppermute(downs[piece][-1], "col", fall))
    return [
        ([parts[piece]] + downs[piece][1:], [None] + ups[piece][1:]) for piece in range(pieces)
    ]


def panel_of(found):
    falling, rising = found
    chips = len(falling)
    held = jnp.stack(
        [falling[0]] + [falling[step] + rising[chips - step] for step in range(1, chips)]
    )
    return held, partner(held)


def after(value, *others):
    return lax.optimization_barrier((value, others))[0]


def scatter_sum(terms, pieces, waits):
    size = lax.axis_size("col")
    chips = size // 2
    up = [None] * pieces
    down = [None] * pieces
    for turn in range(1, chips):
        rise = [(at, at + 2) for at in range(size - 2) if at // 2 <= turn - 1]
        fall = [(at, at - 2) for at in range(2, size) if at // 2 >= chips - turn]
        for piece in range(pieces):
            rising, falling = terms(chips - turn)[piece], terms(turn)[piece]
            if (turn, piece) in waits:
                up[piece], down[piece] = after((up[piece], down[piece]), waits[turn, piece])
            if up[piece] is not None:
                rising, falling = rising + up[piece], falling + down[piece]
            up[piece] = lax.ppermute(rising, "col", rise)
            down[piece] = lax.ppermute(falling, "col", fall)
    return [terms(0)[piece] + up[piece] + down[piece] for piece in range(pieces)]


def smith_step(operator, state, source):
    chips, core = lax.axis_size("col") // 2, lax.axis_index("col") % 2
    every = range(lax.axis_size("row"))

    parts = jnp.split(operator, PIECES, axis=0)
    found = row_panels(parts)
    operator_blocks = spread(parts)
    state_blocks = spread(jnp.split(state, 2, axis=0))

    panels, square, product = [], [], []
    for piece in found:
        panel = panel_of(after(piece, *square, *product))
        square.append(row_product([panel], operator_blocks, every)[0])
        product.append(row_product([panel], state_blocks, every)[0])
        panels.append(panel)
    product = [(piece, partner(piece)) for piece in product]
    first = jnp.stack([block[0] for block in operator_blocks])
    second = jnp.stack([block[1] for block in operator_blocks])
    kept, given = jnp.where(core == 0, first, second), jnp.where(core == 0, second, first)
    came = partner(given)
    groups = []
    for near in range(chips // 2 + 1):
        group = sorted({chips - 1 - near, 1 + near} - set(sum(groups, [])) - {0, chips})
        if near == chips // 2:
            group = [0]
        if group:
            groups.append(group)
    group = sum(groups, [])
    cache = {step: [] for step in group}
    for at, pieces in enumerate(SENT):
        found = term_products(product[at], (kept, came), group, pieces)
        for index, step in enumerate(group):
            cache[step] += found[index * pieces : (index + 1) * pieces]

    square_blocks = spread(square)
    partial = row_product(panels, square_blocks, every[:-1])
    waits = {(2, 0): product[1][0], (3, 0): partial, (2, 1): partial}
    sums = scatter_sum(cache.__getitem__, sum(SENT), waits)
    state_next = jnp.concatenate(sums, axis=0) + source

    cube = row_product(panels, square_blocks, every[-1:], partial)
    cube_blocks = spread(cube)
    partial = row_product(panels, cube_blocks, every[:-1], tile=TILE // 2)
    (operator_fourth,) = row_product(panels, cube_blocks, every[-1:], partial, joined=True)
    return (state_next, operator_fourth)


def solution(mesh):
    in_specs = (P("row", "col"), P("row", "col"), P("row", "col"))
    out_specs = (P("row", "col"), P("row", "col"))
    return jax.shard_map(
        smith_step, mesh=mesh, in_specs=in_specs, out_specs=out_specs, check_vma=False
    )
```
